32 devices in a mesh: rep: 1 (over z), dp: 32 (over x, y, core).
Axes of the slice: x: 4, y: 4, z: 1, core: 2. Of those that a mesh axis runs over, the one named last changes fastest.
The devices are a block of a 4x4x8 slice.
Arguments:
- x: bfloat16 [32, 2048, 512], P(('rep', 'dp'))
- dy: bfloat16 [32, 2048, 512], P(('rep', 'dp'))
- wq: bfloat16 [2, 512, 768], P(None, 'dp')
- wk: bfloat16 [2, 512, 128], P(None, 'dp')
- wv: bfloat16 [2, 512, 128], P(None, 'dp')
- wo: bfloat16 [2, 768, 512], P(None, 'dp')
- w_gate: bfloat16 [2, 512, 2048], P(None, 'dp')
- w_up: bfloat16 [2, 512, 2048], P(None, 'dp')
- w_down: bfloat16 [2, 2048, 512], P(None, 'dp')
Outputs:
- output 1: bfloat16 [32, 2048, 512], P(('rep', 'dp'))
- output 2: bfloat16 [2, 512, 768], P('rep', 'dp')
- output 3: bfloat16 [2, 512, 128], P('rep', 'dp')
- output 4: bfloat16 [2, 512, 128], P('rep', 'dp')
- output 5: bfloat16 [2, 768, 512], P('rep', 'dp')
- output 6: bfloat16 [2, 512, 2048], P('rep', 'dp')
- output 7: bfloat16 [2, 512, 2048], P('rep', 'dp')
- output 8: bfloat16 [2, 2048, 512], P('rep', 'dp')
All inputs are finite; a program needn't handle non-finite values.
Results may differ from the reference program's by a relative error of at most 0.026.
Values are sent between devices in bfloat16 or wider.
A program may use at most 768 MiB of HBM per device.

```python
import jax
import jax.numpy as jnp
from jax import lax

SEQUENCES = 32
TOKENS = 2048
D = 512
HEADS = 6
KV_HEADS = 1
HEAD = 128
FF = 2048
LAYERS = 2
THETA = 10000
NAMES = ("wq", "wk", "wv", "wo", "w_gate", "w_up", "w_down")
SHAPES = {
    "wq": (LAYERS, D, HEADS * HEAD),
    "wk": (LAYERS, D, KV_HEADS * HEAD),
    "wv": (LAYERS, D, KV_HEADS * HEAD),
    "wo": (LAYERS, HEADS * HEAD, D),
    "w_gate": (LAYERS, D, FF),
    "w_up": (LAYERS, D, FF),
    "w_down": (LAYERS, FF, D),
}


def bump(key, n, height):
    away = (jnp.arange(n, dtype=jnp.int32) - jax.random.randint(key, (), 0, n, jnp.int32)) % n
    return jnp.where(away < n // 8, height, 1.0)


def together(key, own, strength):
    shared = jax.random.normal(key, own.shape[1:], jnp.float32)
    return (own + strength * shared) * lax.rsqrt(1 + strength * strength)


def setup_inputs(seed: int = 0, part: int = 0) -> dict:
    kx, kdy, ka, kb, kz, kf, kh, kl, *keys = jax.random.split(jax.random.key(seed), 8 + 3 * len(NAMES))
    kx, kdy, ka, kb = (jax.random.fold_in(k, part) for k in (kx, kdy, ka, kb))
    kw, km, kv = (keys[i::3] for i in range(3))
    shape = (SEQUENCES, TOKENS, D)
    much_x, much_dy = jax.random.uniform(kz, (2,), jnp.float32, 0.0, 1.0)
    loud = 2.0 ** jax.random.uniform(jax.random.fold_in(kz, 1), (), jnp.float32, -1.0, 2.0)
    layers = 2.0 ** jax.random.uniform(kl, (LAYERS, 1, 1), jnp.float32, -1.0, 1.0)
    times = {"wq": 1.0, "wk": 1.0, "wv": 2.0, "wo": layers, "w_gate": 1.0, "w_up": bump(kh, FF, 4.0), "w_down": layers}
    x = together(ka, jax.random.normal(kx, shape, jnp.float32), much_x) * bump(kf, D, 4.0)
    dy = together(kb, jax.random.normal(kdy, shape, jnp.float32), much_dy)
    drawn = {"x": x.astype(jnp.bfloat16), "dy": (loud * dy * (SEQUENCES * TOKENS) ** -0.5).astype(jnp.bfloat16)}
    for key, name in zip(kw, NAMES, strict=True):
        drawn[name] = (jax.random.normal(key, SHAPES[name], jnp.float32) * SHAPES[name][1] ** -0.5 * times[name]).astype(jnp.bfloat16)
    return drawn


def matmul(a, w):
    return jnp.dot(a, w, preferred_element_type=jnp.float32).astype(jnp.bfloat16)


def normed(h):
    wide = h.astype(jnp.float32)
    scale = lax.rsqrt(jnp.mean(wide**2, -1, keepdims=True) + 1e-6)
    return (wide * scale).astype(jnp.bfloat16)


def turned(t, theta):
    half = t.shape[-1] // 2
    angle = jnp.arange(t.shape[0], dtype=jnp.float32)[:, None] * theta ** (-jnp.arange(half, dtype=jnp.float32) / half)
    cos, sin = jnp.cos(angle)[:, None], jnp.sin(angle)[:, None]
    a, b = t[..., :half].astype(jnp.float32), t[..., half:].astype(jnp.float32)
    return jnp.concatenate([a * cos - b * sin, b * cos + a * sin], -1).astype(jnp.bfloat16)


def seen_by(q, k, v):
    tokens, kv = q.shape[0], k.shape[1]
    q = q.reshape(tokens, kv, -1, q.shape[-1])
    scores = jnp.einsum("tgsd,ugd->gstu", q.astype(jnp.float32), k.astype(jnp.float32)) * q.shape[-1] ** -0.5
    place = jnp.arange(tokens)
    weights = jax.nn.softmax(jnp.where(place[:, None] >= place, scores, -jnp.inf), -1).astype(jnp.bfloat16)
    return jnp.einsum("gstu,ugd->tgsd", weights.astype(jnp.float32), v.astype(jnp.float32)).astype(jnp.bfloat16).reshape(tokens, -1)


def layer(h, w):
    a = normed(h)
    q, k = (turned(matmul(a, w[name]).reshape(h.shape[0], -1, HEAD), THETA) for name in ("wq", "wk"))
    h = h + matmul(seen_by(q, k, matmul(a, w["wv"]).reshape(h.shape[0], -1, HEAD)), w["wo"])
    b = normed(h)
    gate = jnp.dot(b, w["w_gate"], preferred_element_type=jnp.float32)
    up = jnp.dot(b, w["w_up"], preferred_element_type=jnp.float32)
    return h + matmul((jax.nn.silu(gate) * up).astype(jnp.bfloat16), w["w_down"])


def stack(weights, h):
    return lax.scan(lambda h, w: (layer(h, w), None), h, weights)[0]


def reference(x, dy, wq, wk, wv, wo, w_gate, w_up, w_down):
    weights = dict(zip(NAMES, (wq, wk, wv, wo, w_gate, w_up, w_down), strict=True))

    def take(so_far, sequence):
        h, by_y = sequence
        _, back = jax.vjp(stack, weights, h)
        by_weights, by_h = back(by_y)
        return jax.tree.map(lambda total, term: total + term.astype(jnp.float32), so_far, by_weights), by_h

    none_yet = {name: jnp.zeros(w.shape, jnp.float32) for name, w in weights.items()}
    by_weights, by_x = lax.scan(take, none_yet, (x, dy))
    return (by_x, *(by_weights[name].astype(jnp.bfloat16) for name in NAMES))
```

```python
import functools

import jax
import jax.numpy as jnp
from jax import lax
from jax.experimental import pallas as pl
from jax.experimental.pallas import tpu as pltpu
from jax.sharding import PartitionSpec as P

HEAD = 128
THETA = 10000
HIDDEN = -2e30
NEG = -1e30
LOG2E = 1.4426950408889634
VMEM = 56 * 2**20
BLOCK = 512
SCALE = HEAD**-0.5
F32 = jnp.float32
LOW = jnp.bfloat16


def _dot(a, b, ca, cb):
    return lax.dot_general(a, b, (((ca,), (cb,)), ((), ())), preferred_element_type=F32)


def _turn(x, cos, sin):
    x = x.astype(F32)
    return (x * cos + pltpu.roll(x, HEAD // 2, 1) * sin).astype(LOW)


def _turn_back(g, cos, sin):
    g = g.astype(LOW).astype(F32)
    return (g * cos - pltpu.roll(g, HEAD // 2, 1) * sin).astype(LOW)


def _causal(keys, queries, ahead):
    return lax.broadcasted_iota(jnp.int32, (keys, queries), 0) <= lax.broadcasted_iota(jnp.int32, (keys, queries), 1) + ahead


def _forward(q_ref, k_ref, v_ref, cos_ref, sin_ref, o_ref, lse_ref, k_s, q_s, top_s, mix_s, *, heads, bq):
    iq = pl.program_id(0)
    e = SCALE * LOG2E

    @pl.when(iq == 0)
    def _():
        k_s[...] = _turn(k_ref[...], cos_ref[...], sin_ref[...])

    mine = pl.ds(pl.multiple_of(iq * bq, bq), bq)
    cos, sin = cos_ref[mine, :], sin_ref[mine, :]
    for n in range(heads):
        q_s[n] = _turn(q_ref[:, n * HEAD : (n + 1) * HEAD], cos, sin)
        top_s[n] = jnp.full((1, bq), NEG, F32)
        mix_s[n] = jnp.zeros((HEAD + 8, bq), F32)

    def block(start, keys, first, masked):
        here = pl.ds(start, keys)
        cols = bq - first
        k = k_s[here, :]
        scores = [_dot(k, q_s[n, first:, :], 1, 1) for n in range(heads)]
        ok = _causal(keys, cols, 0) if masked else None
        weights, keeps = [], []
        for n, s in enumerate(scores):
            if masked:
                s = jnp.where(ok, s, HIDDEN)
            old = top_s[n, :, first:]
            top = jnp.maximum(old, s.max(axis=0, keepdims=True))
            top_s[n, :, first:] = top
            weights.append(jnp.exp2((s - top) * e).astype(LOW))
            keeps.append(jnp.exp2((old - top) * e))
        values = jnp.concatenate([v_ref[here, :].T, jnp.ones((8, keys), LOW)], axis=0)
        for n in range(heads):
            mix_s[n, :, first:] = mix_s[n, :, first:] * keeps[n] + _dot(values, weights[n], 1, 0)

    lax.fori_loop(0, iq, lambda j, _: block(pl.multiple_of(j * bq, bq), bq, 0, False), None)
    half = bq // 2
    base = pl.multiple_of(iq * bq, bq)
    block(base, half, 0, True)
    block(base + half, half, half, True)

    for n in range(heads):
        total = mix_s[n, HEAD : HEAD + 1, :]
        o_ref[:, n * HEAD : (n + 1) * HEAD] = (mix_s[n, :HEAD, :] * (1 / total)).T.astype(LOW)
        lse_ref[n : n + 1, :] = top_s[n] * SCALE + jnp.log(total)


def _backward(q_ref, k_ref, v_ref, o_ref, do_ref, lse_ref, cos_ref, sin_ref, d_ref, k_s, q_s, do_s, dq_s, dk_s, dv_s, *, heads, bq):
    iq = pl.program_id(0)
    e = SCALE * LOG2E

    @pl.when(iq == 0)
    def _():
        k_s[...] = _turn(k_ref[...], cos_ref[...], sin_ref[...])
        dk_s[...] = jnp.zeros_like(dk_s)
        dv_s[...] = jnp.zeros_like(dv_s)

    base = pl.multiple_of(iq * bq, bq)
    mine = pl.ds(base, bq)
    cos, sin = cos_ref[mine, :], sin_ref[mine, :]
    dq_s[...] = jnp.zeros_like(dq_s)
    deltas, lses = [], []
    for n in range(heads):
        lanes = slice(n * HEAD, (n + 1) * HEAD)
        q_s[n] = _turn(q_ref[:, lanes], cos, sin)
        do_s[n] = do_ref[:, lanes]
        deltas.append((do_ref[:, lanes].astype(F32) * o_ref[:, lanes].astype(F32)).T.sum(axis=0, keepdims=True))
        lses.append(lse_ref[n : n + 1, :] * LOG2E)

    def block(start, keys, first, masked):
        here = pl.ds(start, keys)
        k, v = k_s[here, :], v_ref[here, :]
        kt = k.T
        ok = _causal(keys, bq - first, 0) if masked else None

        def ahead(n):
            return _dot(k, q_s[n, first:, :], 1, 1), _dot(v, do_s[n, first:, :], 1, 1)

        coming = [ahead(n) for n in range(min(DEEP, heads))]
        for n in range(heads):
            s, dp = coming[n]
            if n + DEEP < heads:
                coming.append(ahead(n + DEEP))
            p = jnp.exp2(s * e - lses[n][:, first:])
            if masked:
                p = jnp.where(ok, p, 0.0)
            ds = (p * (dp - deltas[n][:, first:])).astype(LOW)
            dv_s[here, :] += _dot(p.astype(LOW), do_s[n, first:, :], 1, 0)
            dk_s[here, :] += _dot(ds, q_s[n, first:, :], 1, 0)
            dq_s[n, :, first:] += _dot(kt, ds, 1, 0)

    lax.fori_loop(0, iq, lambda j, _: block(pl.multiple_of(j * bq, bq), bq, 0, False), None)
    half = bq // 2
    block(base, half, 0, True)
    block(base + half, half, half, True)

    for n in range(heads):
        d_ref[mine, n * HEAD : (n + 1) * HEAD] = _turn_back((dq_s[n] * SCALE).T, cos, sin)

    @pl.when(iq == pl.num_programs(0) - 1)
    def _():
        d_ref[:, heads * HEAD : (heads + 1) * HEAD] = _turn_back(dk_s[...] * SCALE, cos_ref[...], sin_ref[...])
        d_ref[:, (heads + 1) * HEAD :] = dv_s[...].astype(LOW)


DEEP = 3


def _sizes(qkv):
    tokens, width = qkv.shape
    heads = width // HEAD - 2
    return tokens, heads, heads * HEAD, min(BLOCK, tokens)


def _cost(tokens, heads, dots, moved):
    return pl.CostEstimate(flops=dots * heads * tokens * tokens * HEAD, transcendentals=heads * tokens * tokens // 2, bytes_accessed=moved)


def attend(qkv, cos, sin):
    tokens, heads, wide, bq = _sizes(qkv)
    whole = lambda shape, at=0: pl.BlockSpec(shape, lambda i: (0, at))
    return pl.pallas_call(
        functools.partial(_forward, heads=heads, bq=bq),
        grid=(tokens // bq,),
        in_specs=[pl.BlockSpec((bq, wide), lambda i: (i, 0)), whole((tokens, HEAD), heads), whole((tokens, HEAD), heads + 1),
                  whole((tokens, HEAD)), whole((tokens, HEAD))],
        out_specs=[pl.BlockSpec((bq, wide), lambda i: (i, 0)), pl.BlockSpec((heads, bq), lambda i: (0, i))],
        out_shape=[jax.ShapeDtypeStruct((tokens, wide), LOW), jax.ShapeDtypeStruct((heads, tokens), F32)],
        scratch_shapes=[pltpu.VMEM((tokens, HEAD), LOW), pltpu.VMEM((heads, bq, HEAD), LOW), pltpu.VMEM((heads, 1, bq), F32),
                        pltpu.VMEM((heads, HEAD + 8, bq), F32)],
        compiler_params=pltpu.CompilerParams(dimension_semantics=("arbitrary",), vmem_limit_bytes=VMEM),
        cost_estimate=_cost(tokens, heads, 2, qkv.size * 4),
        name="attend",
    )(qkv, qkv, qkv, cos, sin)


def attend_bwd(qkv, out, lse, d_out, cos, sin):
    tokens, heads, wide, bq = _sizes(qkv)
    whole = lambda shape, at=0: pl.BlockSpec(shape, lambda i: (0, at))
    rows = pl.BlockSpec((bq, wide), lambda i: (i, 0))
    return pl.pallas_call(
        functools.partial(_backward, heads=heads, bq=bq),
        grid=(tokens // bq,),
        in_specs=[rows, whole((tokens, HEAD), heads), whole((tokens, HEAD), heads + 1), rows, rows, pl.BlockSpec((heads, bq), lambda i: (0, i)),
                  whole((tokens, HEAD)), whole((tokens, HEAD))],
        out_specs=whole(qkv.shape),
        out_shape=jax.ShapeDtypeStruct(qkv.shape, LOW),
        scratch_shapes=[pltpu.VMEM((tokens, HEAD), LOW), pltpu.VMEM((heads, bq, HEAD), LOW), pltpu.VMEM((heads, bq, HEAD), LOW),
                        pltpu.VMEM((heads, HEAD, bq), F32), pltpu.VMEM((tokens, HEAD), F32), pltpu.VMEM((tokens, HEAD), F32)],
        compiler_params=pltpu.CompilerParams(dimension_semantics=("arbitrary",), vmem_limit_bytes=VMEM),
        cost_estimate=_cost(tokens, heads, 5, qkv.size * 8),
        name="attend_bwd",
    )(qkv, qkv, qkv, out, d_out, lse, cos, sin)


def tables(tokens):
    half = HEAD // 2
    angle = jnp.arange(tokens, dtype=F32)[:, None] * THETA ** (-jnp.arange(half, dtype=F32) / half)
    cos, sin = jnp.cos(angle), jnp.sin(angle)
    return jnp.concatenate([cos, cos], 1), jnp.concatenate([-sin, sin], 1)


def normed(h):
    wide = h.astype(F32)
    scale = lax.rsqrt(jnp.mean(wide**2, -1, keepdims=True) + 1e-6)
    return (wide * scale).astype(LOW)


def matmul(a, w):
    return jnp.dot(a, w, preferred_element_type=F32).astype(LOW)


def by_left(d, w):
    return lax.dot_general(d, w, (((1,), (1,)), ((), ())), preferred_element_type=F32)


def by_right(a, d):
    return lax.dot_general(a, d, (((0,), (0,)), ((), ())), preferred_element_type=F32).astype(LOW)


def _scale(wide):
    return lax.rsqrt(jnp.mean(wide**2, -1, keepdims=True) + 1e-6)


def _chunk(ref, f, unit, d):
    return ref[:, f * unit : (f + 1) * unit, :].reshape(-1, d)


def _rows(ref, f, d):
    per = d // ref.shape[1]
    return ref[f * per : (f + 1) * per].reshape(d, d)


def _mlp(mid_ref, gate_ref, up_ref, down_ref, o_ref, *, unit):
    d = mid_ref.shape[1]
    wide = mid_ref[...].astype(F32)
    b = (wide * _scale(wide)).astype(LOW)
    parts = gate_ref.shape[1] // unit

    def first(f):
        return _dot(b, _chunk(gate_ref, f, unit, d), 1, 0), _dot(b, _chunk(up_ref, f, unit, d), 1, 0)

    coming, total = first(0), None
    for f in range(parts):
        gate, up = coming
        if f + 1 < parts:
            coming = first(f + 1)
        act = (gate * jax.nn.sigmoid(gate) * up).astype(LOW)
        more = _dot(act, _rows(down_ref, f, d), 1, 0)
        total = more if total is None else total + more
    o_ref[...] = mid_ref[...] + total.astype(LOW)


def _mlp_bwd(*refs, unit, n, extra):
    mid_ref, g_ref, out_ref, gate_ref, up_ref, down_ref, wo_ref = refs[:7]
    more_ref = refs[7] if extra else None
    d_mid_ref, d_out_ref, p_ref, gate_s, up_s, down_s, o_s = refs[7 + extra :]
    d = mid_ref.shape[1]
    parts = gate_ref.shape[1] // unit
    own = down_ref.shape[1]
    step = pl.program_id(0)

    @pl.when(step == 0)
    def _():
        gate_s[...] = jnp.zeros_like(gate_s)
        up_s[...] = jnp.zeros_like(up_s)
        down_s[...] = jnp.zeros_like(down_s)
        o_s[...] = jnp.zeros_like(o_s)

    wide = mid_ref[...].astype(F32)
    scale = _scale(wide)
    unit_h = wide * scale
    b = unit_h.astype(LOW)
    g = g_ref[...]
    bt, gt = b.T, g.T

    def first(f):
        return (_dot(b, _chunk(gate_ref, f, unit, d), 1, 0), _dot(b, _chunk(up_ref, f, unit, d), 1, 0), _dot(g, _rows(down_ref, f, d), 1, 1))

    coming, d_b = first(0), None
    for f in range(parts):
        gate, up, d_act = coming
        if f + 1 < parts:
            coming = first(f + 1)
        s = jax.nn.sigmoid(gate)
        silu = gate * s
        act = (silu * up).astype(LOW)
        d_act = d_act.astype(LOW).astype(F32)
        d_up = (d_act * silu).astype(LOW)
        d_gate = (d_act * up * (s * (1 + gate * (1 - s)))).astype(LOW)
        down_s[f] += _dot(gt, act, 1, 0)
        gate_s[f] += _dot(bt, d_gate, 1, 0)
        up_s[f] += _dot(bt, d_up, 1, 0)
        more = _dot(d_gate, _chunk(gate_ref, f, unit, d), 1, 1) + _dot(d_up, _chunk(up_ref, f, unit, d), 1, 1)
        d_b = more if d_b is None else d_b + more
    d_b = d_b.astype(LOW).astype(F32)
    d_mid = g + (scale * (d_b - unit_h * jnp.mean(d_b * unit_h, -1, keepdims=True))).astype(LOW)
    d_mid_ref[...] = d_mid
    d_out_ref[...] = _dot(d_mid, wo_ref[...], 1, 1).astype(LOW)
    o_s[...] += _dot(out_ref[...].T, d_mid, 1, 0)

    @pl.when(step == pl.num_programs(0) - 1)
    def _():
        for f in range(parts):
            p_ref[:, f * unit : (f + 1) * unit, :] = gate_s[f].astype(LOW).reshape(n, unit, d)
            p_ref[:, (parts + f) * unit : (parts + f + 1) * unit, :] = up_s[f].astype(LOW).reshape(n, unit, d)
            per = d // own
            p_ref[f * per : (f + 1) * per, 2 * parts * unit : 2 * parts * unit + own, :] = down_s[f].astype(LOW).T.reshape(per, own, d)
        at = 2 * parts * unit + own
        high = o_s.shape[0] // n
        pad = -high % unit
        d_o = o_s[...].reshape(n, high, d)
        if pad:
            d_o = jnp.concatenate([d_o, jnp.zeros((n, pad, d), F32)], 1)
        p_ref[:, at : at + high + pad, :] = d_o.astype(LOW)
        at += high + pad
        if extra:
            for f in range(more_ref.shape[1] // d):
                p_ref[:, at + f * unit : at + (f + 1) * unit, :] = more_ref[:, f * d : (f + 1) * d].reshape(n, unit, d)


ROWS = 512


def _packed_specs(number, n, parts, unit, own, d):
    once = pl.Buffered(buffer_count=1)
    size = parts * unit
    return [pl.BlockSpec((n, size, d), lambda i, k=k: (0, 3 * number + k, 0), pipeline_mode=once) for k in range(3)]


def mlp(mid, packed, number, unit, ff):
    tokens, d = mid.shape
    n = packed.shape[0]
    block = pl.BlockSpec((min(ROWS, tokens), d), lambda i: (i, 0))
    return pl.pallas_call(
        functools.partial(_mlp, unit=unit),
        grid=(tokens // min(ROWS, tokens),),
        in_specs=[block, *_packed_specs(number, n, ff // d, unit, ff // n, d)],
        out_specs=block,
        out_shape=jax.ShapeDtypeStruct(mid.shape, LOW),
        compiler_params=pltpu.CompilerParams(dimension_semantics=("arbitrary",), vmem_limit_bytes=VMEM),
        cost_estimate=pl.CostEstimate(flops=6 * tokens * d * ff, transcendentals=tokens * ff, bytes_accessed=6 * d * ff + 4 * tokens * d),
        name="mlp",
    )(mid, packed, packed, packed)


def mlp_bwd(mid, g, out, packed, number, wo, more, unit, ff):
    tokens, d = mid.shape
    n, heads = packed.shape[0], out.shape[1]
    parts, own = ff // d, ff // n
    once = pl.Buffered(buffer_count=1)
    rows = min(ROWS, tokens)
    block = pl.BlockSpec((rows, d), lambda i: (i, 0))
    heads_block = pl.BlockSpec((rows, heads), lambda i: (i, 0))
    whole = lambda s: pl.BlockSpec(s, lambda i: (0,) * len(s), pipeline_mode=once)
    extra = [] if more is None else [more]
    high = 2 * parts * unit + own + -(-(heads // n) // unit) * unit + sum(t.shape[1] // d * unit for t in extra)
    return pl.pallas_call(
        functools.partial(_mlp_bwd, unit=unit, n=n, extra=len(extra)),
        grid=(tokens // rows,),
        in_specs=[block, block, heads_block, *_packed_specs(number, n, parts, unit, own, d), whole(wo.shape), *(whole(t.shape) for t in extra)],
        out_specs=[block, heads_block, whole((n, high, d))],
        out_shape=[jax.ShapeDtypeStruct(mid.shape, LOW), jax.ShapeDtypeStruct(out.shape, LOW), jax.ShapeDtypeStruct((n, high, d), LOW)],
        scratch_shapes=[pltpu.VMEM((parts, d, d), F32)] * 3 + [pltpu.VMEM(wo.shape, F32)],
        compiler_params=pltpu.CompilerParams(dimension_semantics=("arbitrary",), vmem_limit_bytes=63 * 2**20),
        cost_estimate=pl.CostEstimate(flops=(16 * ff + 4 * heads) * tokens * d, transcendentals=tokens * ff, bytes_accessed=14 * d * ff + 12 * tokens * d),
        name="mlp_bwd",
    )(mid, g, out, packed, packed, packed, wo, *extra)


def _spread(x_ref, o_ref, held, send_sem, recv_sem, *, n):
    me = lax.axis_index("dp")
    meet(me, n)

    def copy(i):
        return pltpu.make_async_remote_copy(src_ref=x_ref, dst_ref=held.at[me], send_sem=send_sem.at[i], recv_sem=recv_sem.at[i],
                                            device_id={"dp": lax.rem(me + i, n)}, device_id_type=pl.DeviceIdType.MESH)

    def came(i):
        return pltpu.make_async_remote_copy(src_ref=x_ref, dst_ref=held.at[lax.rem(me + n - i, n)], send_sem=send_sem.at[i], recv_sem=recv_sem.at[i],
                                            device_id={"dp": lax.rem(me + i, n)}, device_id_type=pl.DeviceIdType.MESH)

    lax.fori_loop(1, n, lambda i, _: copy(i).start(), None)
    o_ref[me] = x_ref[...]

    def take(i, _):
        came(i).wait_recv()
        at = lax.rem(me + n - i, n)
        o_ref[at] = held[at]

    lax.fori_loop(1, n, take, None)
    lax.fori_loop(1, n, lambda i, _: copy(i).wait_send(), None)


def _collect(x_ref, o_ref, held, total, send_sem, recv_sem, *, n):
    me = lax.axis_index("dp")
    meet(me, n)

    def copy(i):
        to = lax.rem(me + i, n)
        return pltpu.make_async_remote_copy(src_ref=x_ref.at[to], dst_ref=held.at[i], send_sem=send_sem.at[i], recv_sem=recv_sem.at[i],
                                            device_id={"dp": to}, device_id_type=pl.DeviceIdType.MESH)

    lax.fori_loop(1, n, lambda i, _: copy(i).start(), None)
    total[...] = x_ref[me].astype(F32)

    def take(i, _):
        copy(i).wait_recv()
        total[...] += held[i].astype(F32)

    lax.fori_loop(1, n, take, None)
    lax.fori_loop(1, n, lambda i, _: copy(i).wait_send(), None)
    o_ref[...] = total[...].astype(LOW)


def meet(me, n):
    barrier = pltpu.get_barrier_semaphore()

    def greet(i, _):
        pl.semaphore_signal(barrier, inc=1, device_id={"dp": lax.rem(me + i, n)}, device_id_type=pl.DeviceIdType.MESH)

    lax.fori_loop(1, n, greet, None)
    pl.semaphore_wait(barrier, n - 1)


def spread(x, n):
    return pl.pallas_call(
        functools.partial(_spread, n=n),
        in_specs=[pl.BlockSpec(memory_space=pltpu.VMEM)],
        out_specs=pl.BlockSpec(memory_space=pltpu.VMEM),
        out_shape=jax.ShapeDtypeStruct((n, *x.shape), x.dtype),
        scratch_shapes=[pltpu.VMEM((n, *x.shape), x.dtype), pltpu.SemaphoreType.DMA((n,)), pltpu.SemaphoreType.DMA((n,))],
        compiler_params=pltpu.CompilerParams(collective_id=0, has_side_effects=True),
        cost_estimate=pl.CostEstimate(flops=2**33, transcendentals=0, bytes_accessed=2 * n * x.size * 2),
        name="spread",
    )(x)


def collect(x, n):
    return pl.pallas_call(
        functools.partial(_collect, n=n),
        in_specs=[pl.BlockSpec(memory_space=pltpu.VMEM)],
        out_specs=pl.BlockSpec(memory_space=pltpu.VMEM),
        out_shape=jax.ShapeDtypeStruct(x.shape[1:], x.dtype),
        scratch_shapes=[pltpu.VMEM(x.shape, x.dtype), pltpu.VMEM(x.shape[1:], F32), pltpu.SemaphoreType.DMA((n,)), pltpu.SemaphoreType.DMA((n,))],
        compiler_params=pltpu.CompilerParams(collective_id=1, has_side_effects=True),
        cost_estimate=pl.CostEstimate(flops=2**33, transcendentals=0, bytes_accessed=2 * x.size * 2),
        name="collect",
    )(x)


def _plan(shapes, n, unit, d):
    plan, at = [], 0
    for rows, wide in shapes:
        own = rows // n
        steps = wide // d if own == unit else -(-own // unit)
        plan.append((at, steps, own))
        at += steps
    return plan, at


def solution(mesh):
    n = mesh.shape["dp"]

    def own(t, unit, d):
        if t.shape[0] == unit:
            return [t[:, i : i + d] for i in range(0, t.shape[1], d)]
        return [jnp.pad(t, ((0, -t.shape[0] % unit), (0, 0)))]

    def mine(got, shapes, unit, d):
        plan, _ = _plan(shapes, n, unit, d)
        blocks = []
        for at, steps, high in plan:
            t = got[at * unit : (at + steps) * unit]
            blocks.append(jnp.concatenate([t[i * unit : (i + 1) * unit] for i in range(steps)], 1) if high == unit else t[:high])
        return blocks

    def step(x, dy, *shards):
        wq, wk, wv, wo, w_gate, w_up, w_down = shards
        layers, unit, d, ff, high = wq.shape[0], wq.shape[1], wo.shape[2], w_gate.shape[2], wo.shape[1]
        widths = [w.shape[2] for w in (wq, wk, wv)]
        wide = sum(widths)
        qkvs = [jnp.concatenate([wq[i], wk[i], wv[i]], 1) for i in range(layers)]
        rest = [p for i in range(layers) for t in (w_gate[i], w_up[i], w_down[i]) for p in own(t, unit, d)]
        rest += [p for i in range(layers) for p in own(wo[i], unit, d)] + [p for i in range(1, layers) for p in own(qkvs[i], unit, d)]
        early, rest = lax.optimization_barrier((qkvs[0], jnp.concatenate(rest, 0)))
        packed = lax.all_gather(rest, "dp", axis=0)
        w_qkv = [spread(early, n).reshape(-1, wide)]
        at, w_o = layers * 3 * ff // d * unit, []
        for i in range(layers):
            w_o.append(packed[:, at : at + high].reshape(-1, d))
            at += -(-high // unit) * unit
        for i in range(1, layers):
            part = packed[:, at : at + wide // d * unit].reshape(n, wide // d, unit, d)
            w_qkv.append(part.transpose(0, 2, 1, 3).reshape(-1, wide))
            at += wide // d * unit

        cos, sin = tables(x.shape[1])
        h, kept = x[0], []
        for i in range(layers):
            a = normed(h)
            qkv = matmul(a, w_qkv[i])
            out, lse = attend(qkv, cos, sin)
            mid = h + matmul(out, w_o[i])
            kept.append((h, a, qkv, out, lse, mid))
            if i + 1 < layers:
                h = mlp(mid, packed, i, unit, ff)

        g, sums, more, before = dy[0], [None] * layers, None, None
        for i in reversed(range(layers)):
            h, a, qkv, out, lse, mid = kept[i]
            mid, d_out, p = mlp_bwd(mid, g, out, packed, i, w_o[i], more, unit, ff)
            if before is None:
                d_out, p = lax.optimization_barrier((d_out, p))
            else:
                d_out, p, before = lax.optimization_barrier((d_out, p, before))
            shapes = [(n * t.shape[1], t.shape[2]) for t in (w_gate, w_up, w_down, wo)] + ([] if more is None else [more.shape])
            sent = lax.psum_scatter(p, "dp", scatter_dimension=0, tiled=False)
            if i + 1 < layers:
                sums[i + 1][0] = before
            sums[i] = [sent, shapes]
            before = sent
            d_qkv = attend_bwd(qkv, out, lse, d_out, cos, sin)
            more = by_right(a, d_qkv)
            g = mid + jax.vjp(normed, h)[1](by_left(d_qkv, w_qkv[i]).astype(LOW))[0]
        blocks = [mine(sent, shapes, unit, d) for sent, shapes in sums]
        first = [collect(more.reshape(n, unit, -1), n)] + [blocks[i - 1][4] for i in range(1, layers)]
        q, k, v = ([t[:, sum(widths[:i]) : sum(widths[: i + 1])] for t in first] for i in range(3))
        gate, up, down, o = ([t[i] for t in blocks] for i in range(4))
        return (g[None], *(jnp.stack(part) for part in (q, k, v, o, gate, up, down)))

    states, cut = P(("rep", "dp"), None, None), P(None, "dp", None)
    return jax.shard_map(
        step,
        mesh=mesh,
        in_specs=(states, states) + (cut,) * 7,
        out_specs=(states,) + (P("rep", "dp", None),) * 7,
        check_vma=False,
    )
```

```python
import functools

import jax
import jax.numpy as jnp
from jax import lax
from jax.experimental import pallas as pl
from jax.experimental.pallas import tpu as pltpu
from jax.sharding import PartitionSpec as P

HEAD = 128
THETA = 10000
HIDDEN = -2e30
NEG = -1e30
LOG2E = 1.4426950408889634
VMEM = 56 * 2**20
BLOCK = 512
SCALE = HEAD**-0.5
F32 = jnp.float32
LOW = jnp.bfloat16


def _dot(a, b, ca, cb):
    return lax.dot_general(a, b, (((ca,), (cb,)), ((), ())), preferred_element_type=F32)


def _turn(x, cos, sin):
    x = x.astype(F32)
    return (x * cos + pltpu.roll(x, HEAD // 2, 1) * sin).astype(LOW)


def _turn_back(g, cos, sin):
    g = g.astype(LOW).astype(F32)
    return (g * cos - pltpu.roll(g, HEAD // 2, 1) * sin).astype(LOW)


def _causal(keys, queries, ahead):
    return lax.broadcasted_iota(jnp.int32, (keys, queries), 0) <= lax.broadcasted_iota(jnp.int32, (keys, queries), 1) + ahead


def _forward(q_ref, k_ref, v_ref, cos_ref, sin_ref, o_ref, lse_ref, k_s, q_s, top_s, mix_s, *, heads, bq):
    iq = pl.program_id(0)
    e = SCALE * LOG2E

    @pl.when(iq == 0)
    def _():
        k_s[...] = _turn(k_ref[...], cos_ref[...], sin_ref[...])

    mine = pl.ds(pl.multiple_of(iq * bq, bq), bq)
    cos, sin = cos_ref[mine, :], sin_ref[mine, :]
    for n in range(heads):
        q_s[n] = _turn(q_ref[:, n * HEAD : (n + 1) * HEAD], cos, sin)
        top_s[n] = jnp.full((1, bq), NEG, F32)
        mix_s[n] = jnp.zeros((HEAD + 8, bq), F32)

    def block(start, keys, first, masked):
        here = pl.ds(start, keys)
        cols = bq - first
        k = k_s[here, :]
        scores = [_dot(k, q_s[n, first:, :], 1, 1) for n in range(heads)]
        ok = _causal(keys, cols, 0) if masked else None
        weights, keeps = [], []
        for n, s in enumerate(scores):
            if masked:
                s = jnp.where(ok, s, HIDDEN)
            old = top_s[n, :, first:]
            top = jnp.maximum(old, s.max(axis=0, keepdims=True))
            top_s[n, :, first:] = top
            weights.append(jnp.exp2((s - top) * e).astype(LOW))
            keeps.append(jnp.exp2((old - top) * e))
        values = jnp.concatenate([v_ref[here, :].T, jnp.ones((8, keys), LOW)], axis=0)
        for n in range(heads):
            mix_s[n, :, first:] = mix_s[n, :, first:] * keeps[n] + _dot(values, weights[n], 1, 0)

    lax.fori_loop(0, iq, lambda j, _: block(pl.multiple_of(j * bq, bq), bq, 0, False), None)
    half = bq // 2
    base = pl.multiple_of(iq * bq, bq)
    block(base, half, 0, True)
    block(base + half, half, half, True)

    for n in range(heads):
        total = mix_s[n, HEAD : HEAD + 1, :]
        o_ref[:, n * HEAD : (n + 1) * HEAD] = (mix_s[n, :HEAD, :] * (1 / total)).T.astype(LOW)
        lse_ref[n : n + 1, :] = top_s[n] * SCALE + jnp.log(total)


def _backward(q_ref, k_ref, v_ref, o_ref, do_ref, lse_ref, cos_ref, sin_ref, d_ref, k_s, q_s, do_s, dq_s, dk_s, dv_s, *, heads, bq):
    iq = pl.program_id(0)
    e = SCALE * LOG2E

    @pl.when(iq == 0)
    def _():
        k_s[...] = _turn(k_ref[...], cos_ref[...], sin_ref[...])
        dk_s[...] = jnp.zeros_like(dk_s)
        dv_s[...] = jnp.zeros_like(dv_s)

    base = pl.multiple_of(iq * bq, bq)
    mine = pl.ds(base, bq)
    cos, sin = cos_ref[mine, :], sin_ref[mine, :]
    dq_s[...] = jnp.zeros_like(dq_s)
    deltas, lses = [], []
    for n in range(heads):
        lanes = slice(n * HEAD, (n + 1) * HEAD)
        q_s[n] = _turn(q_ref[:, lanes], cos, sin)
        do_s[n] = do_ref[:, lanes]
        deltas.append((do_ref[:, lanes].astype(F32) * o_ref[:, lanes].astype(F32)).T.sum(axis=0, keepdims=True))
        lses.append(lse_ref[n : n + 1, :] * LOG2E)

    def block(start, keys, first, masked):
        here = pl.ds(start, keys)
        k, v = k_s[here, :], v_ref[here, :]
        kt = k.T
        ok = _causal(keys, bq - first, 0) if masked else None

        def ahead(n):
            return _dot(k, q_s[n, first:, :], 1, 1), _dot(v, do_s[n, first:, :], 1, 1)

        coming = [ahead(n) for n in range(min(DEEP, heads))]
        for n in range(heads):
            s, dp = coming[n]
            if n + DEEP < heads:
                coming.append(ahead(n + DEEP))
            p = jnp.exp2(s * e - lses[n][:, first:])
            if masked:
                p = jnp.where(ok, p, 0.0)
            ds = (p * (dp - deltas[n][:, first:])).astype(LOW)
            dv_s[here, :] += _dot(p.astype(LOW), do_s[n, first:, :], 1, 0)
            dk_s[here, :] += _dot(ds, q_s[n, first:, :], 1, 0)
            dq_s[n, :, first:] += _dot(kt, ds, 1, 0)

    lax.fori_loop(0, iq, lambda j, _: block(pl.multiple_of(j * bq, bq), bq, 0, False), None)
    half = bq // 2
    block(base, half, 0, True)
    block(base + half, half, half, True)

    for n in range(heads):
        d_ref[mine, n * HEAD : (n + 1) * HEAD] = _turn_back((dq_s[n] * SCALE).T, cos, sin)

    @pl.when(iq == pl.num_programs(0) - 1)
    def _():
        d_ref[:, heads * HEAD : (heads + 1) * HEAD] = _turn_back(dk_s[...] * SCALE, cos_ref[...], sin_ref[...])
        d_ref[:, (heads + 1) * HEAD :] = dv_s[...].astype(LOW)


DEEP = 3


def _sizes(qkv):
    tokens, width = qkv.shape
    heads = width // HEAD - 2
    return tokens, heads, heads * HEAD, min(BLOCK, tokens)


def _cost(tokens, heads, dots, moved):
    return pl.CostEstimate(flops=dots * heads * tokens * tokens * HEAD, transcendentals=heads * tokens * tokens // 2, bytes_accessed=moved)


def attend(qkv, cos, sin):
    tokens, heads, wide, bq = _sizes(qkv)
    whole = lambda shape, at=0: pl.BlockSpec(shape, lambda i: (0, at))
    return pl.pallas_call(
        functools.partial(_forward, heads=heads, bq=bq),
        grid=(tokens // bq,),
        in_specs=[pl.BlockSpec((bq, wide), lambda i: (i, 0)), whole((tokens, HEAD), heads), whole((tokens, HEAD), heads + 1),
                  whole((tokens, HEAD)), whole((tokens, HEAD))],
        out_specs=[pl.BlockSpec((bq, wide), lambda i: (i, 0)), pl.BlockSpec((heads, bq), lambda i: (0, i))],
        out_shape=[jax.ShapeDtypeStruct((tokens, wide), LOW), jax.ShapeDtypeStruct((heads, tokens), F32)],
        scratch_shapes=[pltpu.VMEM((tokens, HEAD), LOW), pltpu.VMEM((heads, bq, HEAD), LOW), pltpu.VMEM((heads, 1, bq), F32),
                        pltpu.VMEM((heads, HEAD + 8, bq), F32)],
        compiler_params=pltpu.CompilerParams(dimension_semantics=("arbitrary",), vmem_limit_bytes=VMEM),
        cost_estimate=_cost(tokens, heads, 2, qkv.size * 4),
        name="attend",
    )(qkv, qkv, qkv, cos, sin)


def attend_bwd(qkv, out, lse, d_out, cos, sin):
    tokens, heads, wide, bq = _sizes(qkv)
    whole = lambda shape, at=0: pl.BlockSpec(shape, lambda i: (0, at))
    rows = pl.BlockSpec((bq, wide), lambda i: (i, 0))
    return pl.pallas_call(
        functools.partial(_backward, heads=heads, bq=bq),
        grid=(tokens // bq,),
        in_specs=[rows, whole((tokens, HEAD), heads), whole((tokens, HEAD), heads + 1), rows, rows, pl.BlockSpec((heads, bq), lambda i: (0, i)),
                  whole((tokens, HEAD)), whole((tokens, HEAD))],
        out_specs=whole(qkv.shape),
        out_shape=jax.ShapeDtypeStruct(qkv.shape, LOW),
        scratch_shapes=[pltpu.VMEM((tokens, HEAD), LOW), pltpu.VMEM((heads, bq, HEAD), LOW), pltpu.VMEM((heads, bq, HEAD), LOW),
                        pltpu.VMEM((heads, HEAD, bq), F32), pltpu.VMEM((tokens, HEAD), F32), pltpu.VMEM((tokens, HEAD), F32)],
        compiler_params=pltpu.CompilerParams(dimension_semantics=("arbitrary",), vmem_limit_bytes=VMEM),
        cost_estimate=_cost(tokens, heads, 5, qkv.size * 8),
        name="attend_bwd",
    )(qkv, qkv, qkv, out, d_out, lse, cos, sin)


def tables(tokens):
    half = HEAD // 2
    angle = jnp.arange(tokens, dtype=F32)[:, None] * THETA ** (-jnp.arange(half, dtype=F32) / half)
    cos, sin = jnp.cos(angle), jnp.sin(angle)
    return jnp.concatenate([cos, cos], 1), jnp.concatenate([-sin, sin], 1)


def normed(h):
    wide = h.astype(F32)
    scale = lax.rsqrt(jnp.mean(wide**2, -1, keepdims=True) + 1e-6)
    return (wide * scale).astype(LOW)


def matmul(a, w):
    return jnp.dot(a, w, preferred_element_type=F32).astype(LOW)


def by_left(d, w):
    return lax.dot_general(d, w, (((1,), (1,)), ((), ())), preferred_element_type=F32)


def by_right(a, d):
    return lax.dot_general(a, d, (((0,), (0,)), ((), ())), preferred_element_type=F32).astype(LOW)


def _scale(wide):
    return lax.rsqrt(jnp.mean(wide**2, -1, keepdims=True) + 1e-6)


def _chunk(ref, f, unit, d):
    return ref[:, f * unit : (f + 1) * unit, :].reshape(-1, d)


def _rows(ref, f, d):
    per = d // ref.shape[1]
    return ref[f * per : (f + 1) * per].reshape(d, d)


def _mlp(mid_ref, gate_ref, up_ref, down_ref, o_ref, *, unit):
    d = mid_ref.shape[1]
    wide = mid_ref[...].astype(F32)
    b = (wide * _scale(wide)).astype(LOW)
    parts = gate_ref.shape[1] // unit

    def first(f):
        return _dot(b, _chunk(gate_ref, f, unit, d), 1, 0), _dot(b, _chunk(up_ref, f, unit, d), 1, 0)

    coming, total = first(0), None
    for f in range(parts):
        gate, up = coming
        if f + 1 < parts:
            coming = first(f + 1)
        act = (gate * jax.nn.sigmoid(gate) * up).astype(LOW)
        more = _dot(act, _rows(down_ref, f, d), 1, 0)
        total = more if total is None else total + more
    o_ref[...] = mid_ref[...] + total.astype(LOW)


def _mlp_bwd(*refs, unit, n, extra):
    mid_ref, g_ref, out_ref, gate_ref, up_ref, down_ref, wo_ref = refs[:7]
    more_ref = refs[7] if extra else None
    d_mid_ref, d_out_ref, p_ref, gate_s, up_s, down_s, o_s = refs[7 + extra :]
    d = mid_ref.shape[1]
    parts = gate_ref.shape[1] // unit
    own = down_ref.shape[1]
    step = pl.program_id(0)

    @pl.when(step == 0)
    def _():
        gate_s[...] = jnp.zeros_like(gate_s)
        up_s[...] = jnp.zeros_like(up_s)
        down_s[...] = jnp.zeros_like(down_s)
        o_s[...] = jnp.zeros_like(o_s)

    wide = mid_ref[...].astype(F32)
    scale = _scale(wide)
    unit_h = wide * scale
    b = unit_h.astype(LOW)
    g = g_ref[...]
    bt, gt = b.T, g.T

    def first(f):
        return (_dot(b, _chunk(gate_ref, f, unit, d), 1, 0), _dot(b, _chunk(up_ref, f, unit, d), 1, 0), _dot(g, _rows(down_ref, f, d), 1, 1))

    coming, d_b = first(0), None
    for f in range(parts):
        gate, up, d_act = coming
        if f + 1 < parts:
            coming = first(f + 1)
        s = jax.nn.sigmoid(gate)
        silu = gate * s
        act = (silu * up).astype(LOW)
        d_act = d_act.astype(LOW).astype(F32)
        d_up = (d_act * silu).astype(LOW)
        d_gate = (d_act * up * (s * (1 + gate * (1 - s)))).astype(LOW)
        down_s[f] += _dot(gt, act, 1, 0)
        gate_s[f] += _dot(bt, d_gate, 1, 0)
        up_s[f] += _dot(bt, d_up, 1, 0)
        more = _dot(d_gate, _chunk(gate_ref, f, unit, d), 1, 1) + _dot(d_up, _chunk(up_ref, f, unit, d), 1, 1)
        d_b = more if d_b is None else d_b + more
    d_b = d_b.astype(LOW).astype(F32)
    d_mid = g + (scale * (d_b - unit_h * jnp.mean(d_b * unit_h, -1, keepdims=True))).astype(LOW)
    d_mid_ref[...] = d_mid
    d_out_ref[...] = _dot(d_mid, wo_ref[...], 1, 1).astype(LOW)
    o_s[...] += _dot(out_ref[...].T, d_mid, 1, 0)

    @pl.when(step == pl.num_programs(0) - 1)
    def _():
        for f in range(parts):
            p_ref[:, f * unit : (f + 1) * unit, :] = gate_s[f].astype(LOW).reshape(n, unit, d)
            p_ref[:, (parts + f) * unit : (parts + f + 1) * unit, :] = up_s[f].astype(LOW).reshape(n, unit, d)
            per = d // own
            p_ref[f * per : (f + 1) * per, 2 * parts * unit : 2 * parts * unit + own, :] = down_s[f].astype(LOW).T.reshape(per, own, d)
        at = 2 * parts * unit + own
        high = o_s.shape[0] // n
        pad = -high % unit
        d_o = o_s[...].reshape(n, high, d)
        if pad:
            d_o = jnp.concatenate([d_o, jnp.zeros((n, pad, d), F32)], 1)
        p_ref[:, at : at + high + pad, :] = d_o.astype(LOW)
        at += high + pad
        if extra:
            for f in range(more_ref.shape[1] // d):
                p_ref[:, at + f * unit : at + (f + 1) * unit, :] = more_ref[:, f * d : (f + 1) * d].reshape(n, unit, d)


ROWS = 512


def _packed_specs(number, n, parts, unit, own, d):
    once = pl.Buffered(buffer_count=1)
    size = parts * unit
    return [pl.BlockSpec((n, size, d), lambda i, k=k: (0, 3 * number + k, 0), pipeline_mode=once) for k in range(3)]


def mlp(mid, packed, number, unit, ff):
    tokens, d = mid.shape
    n = packed.shape[0]
    block = pl.BlockSpec((min(ROWS, tokens), d), lambda i: (i, 0))
    return pl.pallas_call(
        functools.partial(_mlp, unit=unit),
        grid=(tokens // min(ROWS, tokens),),
        in_specs=[block, *_packed_specs(number, n, ff // d, unit, ff // n, d)],
        out_specs=block,
        out_shape=jax.ShapeDtypeStruct(mid.shape, LOW),
        compiler_params=pltpu.CompilerParams(dimension_semantics=("arbitrary",), vmem_limit_bytes=VMEM),
        cost_estimate=pl.CostEstimate(flops=6 * tokens * d * ff, transcendentals=tokens * ff, bytes_accessed=6 * d * ff + 4 * tokens * d),
        name="mlp",
    )(mid, packed, packed, packed)


def mlp_bwd(mid, g, out, packed, number, wo, more, unit, ff):
    tokens, d = mid.shape
    n, heads = packed.shape[0], out.shape[1]
    parts, own = ff // d, ff // n
    once = pl.Buffered(buffer_count=1)
    rows = min(ROWS, tokens)
    block = pl.BlockSpec((rows, d), lambda i: (i, 0))
    heads_block = pl.BlockSpec((rows, heads), lambda i: (i, 0))
    whole = lambda s: pl.BlockSpec(s, lambda i: (0,) * len(s), pipeline_mode=once)
    extra = [] if more is None else [more]
    high = 2 * parts * unit + own + -(-(heads // n) // unit) * unit + sum(t.shape[1] // d * unit for t in extra)
    return pl.pallas_call(
        functools.partial(_mlp_bwd, unit=unit, n=n, extra=len(extra)),
        grid=(tokens // rows,),
        in_specs=[block, block, heads_block, *_packed_specs(number, n, parts, unit, own, d), whole(wo.shape), *(whole(t.shape) for t in extra)],
        out_specs=[block, heads_block, whole((n, high, d))],
        out_shape=[jax.ShapeDtypeStruct(mid.shape, LOW), jax.ShapeDtypeStruct(out.shape, LOW), jax.ShapeDtypeStruct((n, high, d), LOW)],
        scratch_shapes=[pltpu.VMEM((parts, d, d), F32)] * 3 + [pltpu.VMEM(wo.shape, F32)],
        compiler_params=pltpu.CompilerParams(dimension_semantics=("arbitrary",), vmem_limit_bytes=63 * 2**20),
        cost_estimate=pl.CostEstimate(flops=(16 * ff + 4 * heads) * tokens * d, transcendentals=tokens * ff, bytes_accessed=14 * d * ff + 12 * tokens * d),
        name="mlp_bwd",
    )(mid, g, out, packed, packed, packed, wo, *extra)


def _spread(x_ref, o_ref, held, send_sem, recv_sem, *, n):
    me = lax.axis_index("dp")
    meet(me, n)

    def copy(i):
        return pltpu.make_async_remote_copy(src_ref=x_ref, dst_ref=held.at[me], send_sem=send_sem.at[i], recv_sem=recv_sem.at[i],
                                            device_id={"dp": lax.rem(me + i, n)}, device_id_type=pl.DeviceIdType.MESH)

    def came(i):
        return pltpu.make_async_remote_copy(src_ref=x_ref, dst_ref=held.at[lax.rem(me + n - i, n)], send_sem=send_sem.at[i], recv_sem=recv_sem.at[i],
                                            device_id={"dp": lax.rem(me + i, n)}, device_id_type=pl.DeviceIdType.MESH)

    lax.fori_loop(1, n, lambda i, _: copy(i).start(), None)
    o_ref[me] = x_ref[...]

    def take(i, _):
        came(i).wait_recv()
        at = lax.rem(me + n - i, n)
        o_ref[at] = held[at]

    lax.fori_loop(1, n, take, None)
    lax.fori_loop(1, n, lambda i, _: copy(i).wait_send(), None)


def _collect(x_ref, o_ref, held, total, send_sem, recv_sem, *, n):
    me = lax.axis_index("dp")
    meet(me, n)

    def copy(i):
        to = lax.rem(me + i, n)
        return pltpu.make_async_remote_copy(src_ref=x_ref.at[to], dst_ref=held.at[i], send_sem=send_sem.at[i], recv_sem=recv_sem.at[i],
                                            device_id={"dp": to}, device_id_type=pl.DeviceIdType.MESH)

    lax.fori_loop(1, n, lambda i, _: copy(i).start(), None)
    total[...] = x_ref[me].astype(F32)

    def take(i, _):
        copy(i).wait_recv()
        total[...] += held[i].astype(F32)

    lax.fori_loop(1, n, take, None)
    lax.fori_loop(1, n, lambda i, _: copy(i).wait_send(), None)
    o_ref[...] = total[...].astype(LOW)


def meet(me, n):
    barrier = pltpu.get_barrier_semaphore()

    def greet(i, _):
        pl.semaphore_signal(barrier, inc=1, device_id={"dp": lax.rem(me + i, n)}, device_id_type=pl.DeviceIdType.MESH)

    lax.fori_loop(1, n, greet, None)
    pl.semaphore_wait(barrier, n - 1)


def spread(x, n):
    return pl.pallas_call(
        functools.partial(_spread, n=n),
        in_specs=[pl.BlockSpec(memory_space=pltpu.VMEM)],
        out_specs=pl.BlockSpec(memory_space=pltpu.VMEM),
        out_shape=jax.ShapeDtypeStruct((n, *x.shape), x.dtype),
        scratch_shapes=[pltpu.VMEM((n, *x.shape), x.dtype), pltpu.SemaphoreType.DMA((n,)), pltpu.SemaphoreType.DMA((n,))],
        compiler_params=pltpu.CompilerParams(collective_id=0, has_side_effects=True),
        cost_estimate=pl.CostEstimate(flops=2**33, transcendentals=0, bytes_accessed=2 * n * x.size * 2),
        name="spread",
    )(x)


def collect(x, n):
    return pl.pallas_call(
        functools.partial(_collect, n=n),
        in_specs=[pl.BlockSpec(memory_space=pltpu.VMEM)],
        out_specs=pl.BlockSpec(memory_space=pltpu.VMEM),
        out_shape=jax.ShapeDtypeStruct(x.shape[1:], x.dtype),
        scratch_shapes=[pltpu.VMEM(x.shape, x.dtype), pltpu.VMEM(x.shape[1:], F32), pltpu.SemaphoreType.DMA((n,)), pltpu.SemaphoreType.DMA((n,))],
        compiler_params=pltpu.CompilerParams(collective_id=1, has_side_effects=True),
        cost_estimate=pl.CostEstimate(flops=2**33, transcendentals=0, bytes_accessed=2 * x.size * 2),
        name="collect",
    )(x)


def _fill(wq, wk, wv, wo, gate, up, down, early, *packed, unit, d):
    for i, out in enumerate(packed):
        at = 0
        for ref in (gate, up):
            for c in range(0, ref.shape[2], d):
                out[at : at + unit, :] = ref[i, :, c : c + d]
                at += unit
        out[at : at + down.shape[1], :] = down[i]
        at += down.shape[1]
        high = wo.shape[1]
        o, pad = wo[i], -high % unit
        if pad:
            o = jnp.concatenate([o, jnp.zeros((pad, d), o.dtype)], 0)
        out[at : at + high + pad, :] = o
        at += high + pad
        qkv = jnp.concatenate([wq[i], wk[i], wv[i]], 1)
        if i == 0:
            early[...] = qkv
        else:
            for c in range(0, qkv.shape[1], d):
                out[at : at + unit, :] = qkv[:, c : c + d]
                at += unit


def _settle(first, *refs, layers, unit, d):
    sent, (q, k, v, o, gate, up, down) = refs[:layers], refs[layers:]
    ends = []
    for i, got in enumerate(sent):
        at = 0
        for ref in (gate, up):
            for c in range(0, ref.shape[2], d):
                ref[i, :, c : c + d] = got[at : at + unit, :]
                at += unit
        down[i] = got[at : at + down.shape[1], :]
        at += down.shape[1]
        high = o.shape[1]
        o[i] = got[at : at + high + -high % unit, :][:high]
        ends.append(at + high + -high % unit)
    for i in range(layers):
        if i == 0:
            qkv = first[...]
        else:
            got, at = sent[i - 1], ends[i - 1]
            qkv = jnp.concatenate([got[r : r + unit, :] for r in range(at, got.shape[0], unit)], 1)
        c = 0
        for ref in (q, k, v):
            ref[i] = qkv[:, c : c + ref.shape[2]]
            c += ref.shape[2]


def _small(kernel, name, args, outs):
    return pl.pallas_call(
        kernel,
        in_specs=[pl.BlockSpec(memory_space=pltpu.VMEM)] * len(args),
        out_specs=[pl.BlockSpec(memory_space=pltpu.VMEM)] * len(outs),
        out_shape=[jax.ShapeDtypeStruct(s, LOW) for s in outs],
        cost_estimate=pl.CostEstimate(flops=2**28, transcendentals=0, bytes_accessed=4 * sum(t.size for t in args)),
        name=name,
    )(*args)


def solution(mesh):
    n = mesh.shape["dp"]

    def step(x, dy, *shards):
        wq, wk, wv, wo, w_gate, w_up, w_down = shards
        layers, unit, d, ff, high = wq.shape[0], wq.shape[1], wo.shape[2], w_gate.shape[2], wo.shape[1]
        wide = wq.shape[2] + wk.shape[2] + wv.shape[2]
        mlp_rows = 2 * ff // d * unit + w_down.shape[1]
        base, qkv_rows = mlp_rows + high + -high % unit, wide // d * unit
        sizes = [(base + (qkv_rows if i else 0), d) for i in range(layers)]
        early, *rest = _small(functools.partial(_fill, unit=unit, d=d), "fill", shards, [(unit, wide), *sizes])
        packed = [lax.all_gather(rest[0], "dp", axis=0)]
        first = spread(early, n)
        first, *rest = lax.optimization_barrier((first, *rest[1:]))
        packed += [lax.all_gather(t, "dp", axis=0) for t in rest]
        w_o = [t[:, mlp_rows : mlp_rows + high].reshape(-1, d) for t in packed]
        w_qkv = [first.reshape(-1, wide)]
        for t in packed[1:]:
            part = t[:, base : base + qkv_rows].reshape(n, wide // d, unit, d)
            w_qkv.append(part.transpose(0, 2, 1, 3).reshape(-1, wide))

        cos, sin = tables(x.shape[1])
        h, kept = x[0], []
        for i in range(layers):
            a = normed(h)
            qkv = matmul(a, w_qkv[i])
            out, lse = attend(qkv, cos, sin)
            mid = h + matmul(out, w_o[i])
            kept.append((h, a, qkv, out, lse, mid))
            if i + 1 < layers:
                h = mlp(mid, packed[i], 0, unit, ff)

        g, sent, more, before = dy[0], [None] * layers, None, None
        for i in reversed(range(layers)):
            h, a, qkv, out, lse, mid = kept[i]
            mid, d_out, p = mlp_bwd(mid, g, out, packed[i], 0, w_o[i], more, unit, ff)
            if before is None:
                d_out, p = lax.optimization_barrier((d_out, p))
            else:
                d_out, p, before = lax.optimization_barrier((d_out, p, before))
                sent[i + 1] = before
            sent[i] = before = lax.psum_scatter(p, "dp", scatter_dimension=0, tiled=False)
            d_qkv = attend_bwd(qkv, out, lse, d_out, cos, sin)
            more = by_right(a, d_qkv)
            g = mid + jax.vjp(normed, h)[1](by_left(d_qkv, w_qkv[i]).astype(LOW))[0]
        mine = collect(more.reshape(n, unit, -1), n)
        done = _small(functools.partial(_settle, layers=layers, unit=unit, d=d), "settle", [mine, *sent], [t.shape for t in shards])
        return (g[None], *done)

    states, cut = P(("rep", "dp"), None, None), P(None, "dp", None)
    return jax.shard_map(
        step,
        mesh=mesh,
        in_specs=(states, states) + (cut,) * 7,
        out_specs=(states,) + (P("rep", "dp", None),) * 7,
        check_vma=False,
    )
```
